32 devices in a mesh: cx: 4 (over z), cy: 2 (over y), tp: 4 (over x, core).
Axes of the slice: x: 2, y: 2, z: 4, core: 2. Of those that a mesh axis runs over, the one named last changes fastest.
Arguments:
- neighbor_ids: int32 [16, 8, 128], P(('cx', 'cy'), 'tp'), may hold values from 0 to 1023
- decoder: bfloat16 [16, 64, 896], P(('cx', 'cy')), may hold values from -6 to 6
- table: bfloat16 [1024, 896], P(('cx', 'cy')), may hold values from -6 to 6
- attn_in: bfloat16 [6, 896, 896], P(None, ('cx', 'cy'), 'tp'), may hold values from -0.1875 to 0.1875
- attn_out: bfloat16 [2, 896, 896], P(None, 'tp', ('cx', 'cy')), may hold values from -0.1875 to 0.1875
- gains: float32 [3, 896], replicated, may hold values from 0.25 to 1.75
- w_up: bfloat16 [896, 3584], P(('cx', 'cy'), 'tp'), may hold values from -0.1875 to 0.1875
- w_down: bfloat16 [3584, 896], P('tp', ('cx', 'cy')), may hold values from -0.09375 to 0.09375
Outputs:
- encoded: bfloat16 [16, 8, 128, 896], P(('cx', 'cy'), 'tp')
The draws below stay inside these ranges and needn't reach their ends.
All inputs are finite; a program needn't handle non-finite values.
Results may differ from the reference program's by a relative error of at most 0.013.
Values may be sent and summed in bfloat16 or wider, within the bound.
No kernel may reach another device: no remote copies, remote signals or barrier semaphores. Data moves between devices by JAX's collectives and lax.ppermute only.
A program may use at most 128 MiB of HBM per device.

```python
import math
import jax
import jax.numpy as jnp
import numpy as np
from jax import lax

D = 896
HD = 64
FF = 3584
VOCAB = 1024
L = 128
M = 64
SPANS = 16
NBR = 8


def set_ends(array, rng, low, largest):
    place = [jax.random.randint(jax.random.fold_in(rng, axis), (), 0, length) for axis, length in enumerate(array.shape)]
    main_axis = array.shape.index(max(array.shape))
    next_to = place[:main_axis] + [(place[main_axis] + 1) % array.shape[main_axis]] + place[main_axis + 1:]
    return array.at[tuple(place)].set(low).at[tuple(next_to)].set(largest)


def levels(rng, extent, split, least, high):
    loudness, own = 1.0, jax.random.fold_in(rng, 6)
    for axis_at, blocks in split:
        heights = jnp.exp(jax.random.uniform(jax.random.fold_in(own, axis_at), (blocks,), jnp.float32, least / len(split), high / len(split)))
        loudness = loudness * jnp.repeat(heights, extent[axis_at] // blocks).reshape([-1 if axis == axis_at else 1 for axis in range(len(extent))])
    return loudness


def rank_bounds(amount, lean):
    loads = [(1 << 20) // math.isqrt(standing ** lean) + 1 for standing in range(1, amount + 1)]
    deviation = 1 + sum(loads) // (1 << 30)
    return np.cumsum(np.array([max(1, weight // deviation) for weight in loads]))


def ranked(stream_key, shape, amount, slope):
    grid = rank_bounds(amount, slope)
    lot = jax.random.randint(jax.random.fold_in(stream_key, 1), shape, 0, int(grid[amount - 1]))
    grade = jnp.searchsorted(jnp.asarray(grid, jnp.int32), lot, side="right")
    return jax.random.permutation(jax.random.fold_in(stream_key, 2), amount)[grade].astype(jnp.int32)


def bell_draw(stream_key, shape, scale, limit, cuts=(), held_as=jnp.bfloat16):
    array = jax.random.normal(stream_key, shape, jnp.float32) * scale
    if len(cuts) > 0:
        array = levels(stream_key, shape, cuts, -0.22, 0.18) * array
    return jnp.clip(array, min=-limit, max=limit).astype(held_as)


def setup_inputs(seed: int = 0) -> dict:
    seeds = jax.random.split(jax.random.key(seed), 9)
    neighbor_ids = set_ends(ranked(seeds[0], (SPANS, NBR, L), VOCAB, 2), jax.random.fold_in(seeds[0], 3), 0, VOCAB - 1).astype(jnp.int32)
    decoder = bell_draw(seeds[1], (SPANS, M, D), 1.0, 6.0, ((0, 8),))
    table = bell_draw(seeds[2], (VOCAB, D), 1.0, 6.0, ((0, 8),))
    attn_in = bell_draw(seeds[3], (6, D, D), D ** -0.5, 0.1875, ((1, 8), (2, 4)))
    attn_out = bell_draw(seeds[4], (2, D, D), D ** -0.5, 0.1875, ((1, 4), (2, 8)))
    gains = jnp.clip(1.0 + 0.15 * jax.random.normal(seeds[5], (3, D), jnp.float32), 0.25, 1.75)
    w_up = bell_draw(seeds[6], (D, FF), D ** -0.5, 0.1875, ((0, 8), (1, 4)))
    w_down = bell_draw(seeds[7], (FF, D), FF ** -0.5, 0.09375, ((0, 4), (1, 8)))
    return {"neighbor_ids": neighbor_ids, "decoder": decoder, "table": table, "attn_in": attn_in, "attn_out": attn_out, "gains": gains, "w_up": w_up, "w_down": w_down}


def layer_norm(values, gain):
    middle = lax.optimization_barrier(jnp.mean(values, axis=-1, keepdims=True))
    centred = values - middle
    spread = lax.optimization_barrier(jnp.mean(centred * centred, axis=-1, keepdims=True))
    return (centred * lax.rsqrt(spread + 1e-05) * gain).astype(jnp.bfloat16)

def project(hidden, matrix):
    return jnp.dot(hidden, matrix, preferred_element_type=jnp.float32).astype(jnp.bfloat16)

def attend(query, key_rows, value_rows):
    batch, q_len, width = query.shape
    k_len = key_rows.shape[1]
    heads = width // HD
    q_heads = query.reshape(batch, q_len, heads, HD).astype(jnp.float32)
    k_heads = key_rows.reshape(batch, k_len, heads, HD).astype(jnp.float32)
    v_heads = value_rows.reshape(batch, k_len, heads, HD).astype(jnp.float32)
    scores = jnp.einsum('bqhd,bkhd->bhqk', q_heads, k_heads) * HD ** (-0.5)
    probs = jax.nn.softmax(scores, axis=-1).astype(jnp.bfloat16).astype(jnp.float32)
    mixed = jnp.einsum('bhqk,bkhd->bqhd', probs, v_heads)
    return mixed.reshape(batch, q_len, width).astype(jnp.bfloat16)

def reference(neighbor_ids, decoder, table, attn_in, attn_out, gains, w_up, w_down):

    def one_span(item):
        ids, dec = item
        x_zero = table[ids.reshape(-1)].astype(jnp.float32)
        h_one = layer_norm(x_zero, gains[0])
        query = project(h_one, attn_in[0]).reshape(NBR, L, D)
        keys = project(h_one, attn_in[1]).reshape(NBR, L, D)
        values = project(h_one, attn_in[2]).reshape(NBR, L, D)
        self_out = attend(query, keys, values).reshape(NBR * L, D)
        x_one = x_zero + jnp.dot(self_out, attn_out[0], preferred_element_type=jnp.float32)
        h_two = layer_norm(x_one, gains[1])
        cross_q = project(h_two, attn_in[3]).reshape(1, NBR * L, D)
        cross_k = project(dec, attn_in[4]).reshape(1, M, D)
        cross_v = project(dec, attn_in[5]).reshape(1, M, D)
        cross = attend(cross_q, cross_k, cross_v).reshape(NBR * L, D)
        x_two = x_one + jnp.dot(cross, attn_out[1], preferred_element_type=jnp.float32)
        h_three = layer_norm(x_two, gains[2])
        upward = jnp.dot(h_three, w_up, preferred_element_type=jnp.float32)
        act = jax.nn.gelu(upward, approximate=True).astype(jnp.bfloat16)
        mixed = jnp.dot(act, w_down, preferred_element_type=jnp.float32)
        return (x_two + mixed).astype(jnp.bfloat16).reshape(NBR, L, D)
    return lax.map(one_span, (neighbor_ids, decoder))
```

```python
import functools

import jax
import jax.numpy as jnp
from jax import lax
from jax.experimental import pallas as pl
from jax.experimental.pallas import tpu as pltpu
from jax.sharding import PartitionSpec as P

HD = 64
LANES = 128
MIB = 1024 * 1024
NT = (((1,), (1,)), ((), ()))


def layer_norm(values, gain):
    middle = jnp.mean(values, axis=-1, keepdims=True)
    centred = values - middle
    spread = jnp.mean(centred * centred, axis=-1, keepdims=True)
    return (centred * lax.rsqrt(spread + 1e-05) * gain).astype(jnp.bfloat16)


def dot(a, b):
    return jnp.dot(a, b, preferred_element_type=jnp.float32)


def dot_nt(a, b):
    return lax.dot_general(a, b, NT, preferred_element_type=jnp.float32)


def kernel_norm(values, gain):
    centred = values - jnp.mean(values, axis=-1, keepdims=True)
    scaled = centred * lax.rsqrt(jnp.mean(centred * centred, axis=-1, keepdims=True) + 1e-05)
    scaled = scaled.reshape(-1, *gain.shape) * gain
    return scaled.reshape(values.shape).astype(jnp.bfloat16)


def joined(parts):
    return jnp.concatenate(parts, axis=1)


def project(hidden, matrix):
    return dot(hidden, matrix).astype(jnp.bfloat16)


def attend(query, key_rows, value_rows):
    batch, q_len, width = query.shape
    k_len = key_rows.shape[1]
    heads = width // HD
    q_heads = query.reshape(batch, q_len, heads, HD)
    k_heads = key_rows.reshape(batch, k_len, heads, HD)
    v_heads = value_rows.reshape(batch, k_len, heads, HD)
    scores = jnp.einsum("bqhd,bkhd->bhqk", q_heads, k_heads, preferred_element_type=jnp.float32) * HD ** (-0.5)
    probs = jax.nn.softmax(scores, axis=-1).astype(jnp.bfloat16)
    mixed = jnp.einsum("bhqk,bkhd->bqhd", probs, v_heads, preferred_element_type=jnp.float32)
    return mixed.reshape(batch, q_len, width).astype(jnp.bfloat16)


def general_body(neighbor_ids, decoder, table, attn_in, attn_out, gains, w_up, w_down):
    full_table = lax.all_gather(table, ("cx", "cy"), axis=0, tiled=True)
    in_w = lax.all_gather(attn_in, ("cx", "cy"), axis=1, tiled=True)
    out_w = lax.all_gather(attn_out, ("cx", "cy"), axis=2, tiled=True)
    up_w = lax.all_gather(w_up, ("cx", "cy"), axis=0, tiled=True)
    down_w = lax.all_gather(w_down, ("cx", "cy"), axis=1, tiled=True)
    spans, nbrs, length = neighbor_ids.shape
    width = full_table.shape[1]
    dec_len = decoder.shape[1]
    total = spans * nbrs * length
    dec_rows = decoder.reshape(spans * dec_len, width)
    x_zero = jnp.take(full_table, neighbor_ids.reshape(-1), axis=0).astype(jnp.float32)
    h_one = layer_norm(x_zero, gains[0])
    in_full = lax.all_gather(in_w, "tp", axis=2, tiled=True)
    out_full = lax.all_gather(out_w, "tp", axis=1, tiled=True)
    query, keys, values = (project(h_one, in_full[i]).reshape(spans * nbrs, length, width) for i in range(3))
    self_out = attend(query, keys, values).reshape(total, width)
    x_one = x_zero + dot(self_out, out_full[0])
    h_two = layer_norm(x_one, gains[1])
    cross_q = project(h_two, in_full[3]).reshape(spans, nbrs * length, width)
    cross_k, cross_v = (project(dec_rows, in_full[i]).reshape(spans, dec_len, width) for i in (4, 5))
    cross = attend(cross_q, cross_k, cross_v).reshape(total, width)
    x_two = x_one + dot(cross, out_full[1])
    every = lax.all_gather(layer_norm(x_two, gains[2]), "tp", axis=0, tiled=True)
    act = jax.nn.gelu(dot(every, up_w), approximate=True).astype(jnp.bfloat16)
    mixed = lax.psum_scatter(dot(act, down_w).astype(jnp.bfloat16), "tp", scatter_dimension=0, tiled=True)
    return (x_two + mixed.astype(jnp.float32)).astype(jnp.bfloat16).reshape(spans, nbrs, length, width)


def group_of(pos_ref, dy, k):
    return jnp.bitwise_xor(pos_ref[0], k) * 2 + jnp.bitwise_xor(pos_ref[1], dy)


def single(refs):
    return [(ref, i) for ref in refs for i in range(ref.shape[0])]


def pack_kernel(nz, trows, pos_ref, *refs):
    blocks, out_ref = single(refs[:-1]), refs[-1]
    rows = refs[0].shape[1] - trows
    head = trows * 2 * nz
    for n, (ref, i) in enumerate(blocks):
        dx, dy = n // nz % 2, n // nz // 2
        group = group_of(pos_ref, dy, n % nz)
        out_ref[dx, pl.ds(pl.multiple_of(head + group * rows, 16), rows)] = ref[i, trows:trows + rows]
        if trows:
            out_ref[dx, pl.ds(pl.multiple_of(group * trows, 16), trows)] = ref[i, 0:trows]


def qkv_kernel(pos_ref, ids_ref, gains_ref, own, other, x0_ref, q_s, k_s, v_s, tab, wts):
    total, width = x0_ref.shape
    groups, tps, trows = tab.shape[:3]
    slab = width // tps
    for n in range(tps):
        src, tp = (own, other)[n % 2], jnp.bitwise_xor(pos_ref[2], n)
        for g in range(groups):
            tab[g, tp] = src[n // 2, g * trows:(g + 1) * trows]
        wts[tp] = src[n // 2, groups * trows:]
    vocab = groups * tps * trows
    spots = lax.broadcasted_iota(jnp.int32, (total, vocab), 1)
    chosen = jnp.where(spots == ids_ref[...], 1.0, 0.0).astype(jnp.bfloat16)
    x_zero = dot(chosen, tab[...].reshape(vocab, width))
    x0_ref[...] = x_zero.astype(jnp.bfloat16)
    hidden = kernel_norm(x_zero, gains_ref[0])
    parts = [dot(hidden, wts[tp, :, 0:3 * slab]).astype(jnp.bfloat16) for tp in range(tps)]
    for at, ref in enumerate((q_s, k_s, v_s)):
        ref[...] = joined([part[:, at * slab:(at + 1) * slab] for part in parts])


def self_kernel(seqs, length, q_s, k_s, v_s, out_ref):
    width = q_s.shape[1]
    left = lax.broadcasted_iota(jnp.int32, (length, LANES), 1) < HD

    def one(seq, carry):
        own = pl.ds(pl.multiple_of(seq * length, length), length)
        for tile in range(width // LANES):
            lanes = slice(tile * LANES, (tile + 1) * LANES)
            query, keys, values = q_s[own, lanes], k_s[own, lanes], v_s[own, lanes]
            zero = jnp.zeros_like(query)
            both = jnp.concatenate([jnp.where(left, query, zero), jnp.where(left, zero, query)], axis=0)
            scores = dot_nt(both, keys) * HD ** (-0.5)
            grown = jnp.exp(scores - jnp.max(scores, axis=-1, keepdims=True))
            probs = (grown / jnp.sum(grown, axis=-1, keepdims=True)).astype(jnp.bfloat16)
            mixed = dot(probs, values)
            out_ref[own, lanes] = jnp.where(left, mixed[:length], mixed[length:]).astype(jnp.bfloat16)
        return carry

    lax.fori_loop(0, seqs, one, 0)


def mid_kernel(pos_ref, gains_ref, dec_ref, x0_ref, self_ref, ta_own, ta_other, own, other,
               x1_ref, q_s, k_s, v_s, o1, wts, cqw, o0):
    _, width = x0_ref.shape
    tps, tail = wts.shape[0], cqw.shape[2]
    slab = width // tps
    for n in range(tps):
        tp = jnp.bitwise_xor(pos_ref[2], n)
        wts[tp] = (own, other)[n % 2][n // 2]
        cqw[tp] = (ta_own, ta_other)[n % 2][n // 2, ta_own.shape[1] - width:, width - tail:]
    for at, ref in ((2, o0), (3, o1)):
        ref[...] = joined([wts[tp, :, at * slab:(at + 1) * slab] for tp in range(tps)])
    parts = [dot(dec_ref[...], wts[tp, :, 0:2 * slab]).astype(jnp.bfloat16) for tp in range(tps)]
    k_s[...] = joined([part[:, 0:slab] for part in parts])
    v_s[...] = joined([part[:, slab:2 * slab] for part in parts])
    x_one = x0_ref[...].astype(jnp.float32) + dot_nt(self_ref[...], o0[...])
    hidden = kernel_norm(x_one, gains_ref[1])
    q_s[...] = joined([dot(hidden, cqw[tp]).astype(jnp.bfloat16)[:, tail - slab:] for tp in range(tps)])
    x1_ref[...] = x_one


def cross_kernel(spans, gains_ref, x1_ref, q_s, k_s, v_s, o1, x2_ref, h3_ref, c_s):
    total, width = x1_ref.shape
    dec_len, per_span = k_s.shape[0] // spans, total // spans
    left_keys = lax.broadcasted_iota(jnp.int32, (dec_len, LANES), 1) < HD
    left = lax.broadcasted_iota(jnp.int32, (per_span, 2 * dec_len), 1) < dec_len
    for span in range(spans):
        own = slice(span * per_span, (span + 1) * per_span)
        theirs = slice(span * dec_len, (span + 1) * dec_len)
        for tile in range(width // LANES):
            lanes = slice(tile * LANES, (tile + 1) * LANES)
            keys, values = k_s[theirs, lanes], v_s[theirs, lanes]
            zero = jnp.zeros_like(keys)
            keys = jnp.concatenate([jnp.where(left_keys, keys, zero), jnp.where(left_keys, zero, keys)], axis=0)
            values = jnp.concatenate([jnp.where(left_keys, values, zero), jnp.where(left_keys, zero, values)], axis=0)
            scores = dot_nt(q_s[own, lanes], keys) * HD ** (-0.5)
            top_a = jnp.max(jnp.where(left, scores, -jnp.inf), axis=-1, keepdims=True)
            top_b = jnp.max(jnp.where(left, -jnp.inf, scores), axis=-1, keepdims=True)
            grown = jnp.exp(scores - jnp.where(left, top_a, top_b))
            sum_a = jnp.sum(jnp.where(left, grown, 0.0), axis=-1, keepdims=True)
            sum_b = jnp.sum(jnp.where(left, 0.0, grown), axis=-1, keepdims=True)
            probs = (grown / jnp.where(left, sum_a, sum_b)).astype(jnp.bfloat16)
            c_s[own, lanes] = dot(probs, values).astype(jnp.bfloat16)
    x_two = x1_ref[...] + dot_nt(c_s[...], o1[...])
    x2_ref[...] = x_two
    h3_ref[...] = kernel_norm(x_two, gains_ref[2])


def mlp_kernel(nz, given, halves, add, pos_ref, *refs):
    blocks, refs = single(refs[:given]), refs[given:]
    hiddens, refs = refs[:halves], refs[halves:]
    before, refs = (refs[:halves], refs[halves:]) if add else ((None,) * halves, refs)
    outs, (up, down) = refs[:halves], refs[halves:]
    rows = up.shape[0] // (2 * nz)
    for n, (ref, i) in enumerate(blocks):
        to = pl.ds(pl.multiple_of(group_of(pos_ref, n // nz, n % nz) * rows, 16), rows)
        up[to] = ref[i, 0:rows]
        down[to] = ref[i, rows:2 * rows]
    for half in range(halves):
        act = jax.nn.gelu(dot(hiddens[half][...], up[...]), approximate=True).astype(jnp.bfloat16)
        more = dot_nt(act, down[...])
        outs[half][...] = (more if before[half] is None else before[half][...] + more).astype(outs[half].dtype)


VMEM = pl.BlockSpec(memory_space=pltpu.VMEM)
SMEM = pl.BlockSpec(memory_space=pltpu.SMEM)


def kernel_call(kernel, specs, outs, scratch, flops, mib):
    return pl.pallas_call(
        kernel,
        out_shape=outs,
        in_specs=specs,
        out_specs=jax.tree.map(lambda _: VMEM, outs),
        scratch_shapes=scratch,
        compiler_params=pltpu.CompilerParams(vmem_limit_bytes=mib * MIB),
        cost_estimate=pl.CostEstimate(flops=flops, bytes_accessed=1 << 23, transcendentals=0),
    )


def permute(value, axis, size, flip):
    return lax.ppermute(value, axis, [(i, i ^ flip) for i in range(size)])


def spread(block, nz, step, near):
    if step == 2:
        block = jnp.concatenate([block, permute(block, "cx", nz, 1)])
    at = range(0, nz, step)

    def sent(found, n, source, axis, size, flip):
        if near and at[n] == 1:
            return permute(found[0], "cx", nz, 1)
        return permute(source[n], axis, size, flip)

    line = [block if k == 0 else permute(block, "cx", nz, k) for k in at]
    over_x, over_y, both = [], [], []
    for n in range(len(at)):
        over_x.append(sent(over_x, n, line, "tp", 4, 2))
        over_y.append(sent(over_y, n, line, "cy", 2, 1))
    for n in range(len(at)):
        if n % 2 == 0:
            both.append(sent(both, n, over_y, "tp", 4, 2))
        else:
            both.append(sent(both, n, over_x, "cy", 2, 1))
    return line, over_x, over_y, both


def fast_body(nz, neighbor_ids, decoder, table, attn_in, attn_out, gains, w_up, w_down):
    bf16, f32 = jnp.bfloat16, jnp.float32
    spans, nbrs, length = neighbor_ids.shape
    width = decoder.shape[2]
    total, seqs = spans * nbrs * length, spans * nbrs
    tps = 4
    trows = table.shape[0] // tps
    slab = attn_in.shape[2]
    wide = w_up.shape[1]
    vocab = table.shape[0] * 2 * nz
    where = [lax.axis_index(a) for a in ("cx", "cy", "tp")]
    pos = jnp.stack(where).astype(jnp.int32)
    gains = jnp.broadcast_to(gains[:, None], (gains.shape[0], 8, width))

    ta = jnp.concatenate(
        [
            lax.dynamic_slice_in_dim(table, where[2] * trows, trows, 0),
            jnp.concatenate([attn_in[i] for i in range(4)], axis=1),
        ],
        axis=0,
    )
    bb = jnp.concatenate([attn_in[4], attn_in[5], attn_out[0].T, attn_out[1].T], axis=1)
    ud = jnp.concatenate([w_up, w_down.T], axis=0)

    def shared(block, head, step):
        blocks = sum(spread(block[None], nz, step, False), [])
        packed = kernel_call(
            functools.partial(pack_kernel, nz, head),
            [SMEM] + [VMEM] * len(blocks),
            jax.ShapeDtypeStruct((2, 2 * nz * block.shape[0], width), bf16),
            [],
            1 << 20,
            12,
        )(pos, *blocks)
        return packed, permute(packed, "tp", tps, 1)

    ta_all = shared(ta, trows, 1)
    bb_all = shared(bb, 0, 2)
    ud_line, ud_x, ud_y, ud_both = spread(ud[None], nz, 1, True)

    rows_of = lambda dtype: jax.ShapeDtypeStruct((total, width), dtype)
    x_zero, *qkv = kernel_call(
        qkv_kernel,
        [SMEM] + [VMEM] * 4,
        tuple(rows_of(bf16) for _ in range(4)),
        [pltpu.VMEM((2 * nz, tps, trows, width), bf16), pltpu.VMEM((tps, width, width), bf16)],
        2 * total * width * (3 * width + vocab),
        36,
    )(pos, neighbor_ids.reshape(total, 1), gains, *ta_all)
    self_out = kernel_call(
        functools.partial(self_kernel, seqs, length), [VMEM] * 3, rows_of(bf16), [], 4 * total * width * length, 12
    )(*qkv)

    tail = -(-slab // LANES) * LANES
    dec_rows = decoder.reshape(-1, width)
    dec_of = jax.ShapeDtypeStruct(dec_rows.shape, bf16)
    x_one, *cross_qkvo = kernel_call(
        mid_kernel,
        [SMEM] + [VMEM] * 8,
        (rows_of(f32), rows_of(bf16), dec_of, dec_of, jax.ShapeDtypeStruct((width, width), bf16)),
        [
            pltpu.VMEM((tps, width, width), bf16),
            pltpu.VMEM((tps, width, tail), bf16),
            pltpu.VMEM((width, width), bf16),
        ],
        2 * total * width * 3 * width,
        40,
    )(pos, gains, dec_rows, x_zero, self_out, *ta_all, *bb_all)
    x_two, h_three = kernel_call(
        functools.partial(cross_kernel, spans),
        [VMEM] * 6,
        (rows_of(f32), rows_of(bf16)),
        [pltpu.VMEM((total, width), bf16)],
        2 * total * width * width,
        16,
    )(gains, x_one, *cross_qkvo)

    h_other = permute(h_three, "tp", tps, 1)
    scratch = [
        pltpu.VMEM((width, wide), bf16),
        pltpu.VMEM((width, wide), bf16),
    ]

    def mlp(blocks, hiddens, before, dtypes):
        return kernel_call(
            functools.partial(mlp_kernel, nz, len(blocks), len(hiddens), bool(before)),
            [SMEM] + [VMEM] * len(blocks) + [VMEM] * (len(hiddens) + len(before)),
            tuple(rows_of(dtype) for dtype in dtypes),
            scratch,
            4 * total * width * wide * len(hiddens),
            20,
        )(pos, *blocks, *hiddens, *before)

    part_other, part_own = mlp(ud_line + ud_y, (h_other, h_three), (), (f32, f32))
    (theirs,) = mlp(ud_x + ud_both, (h_other,), (part_other,), (bf16,))
    from_other = permute(theirs, "tp", tps, 1)
    (ours,) = mlp(ud_x + ud_both, (h_three,), (part_own,), (f32,))
    return (x_two + ours + from_other.astype(f32)).astype(bf16).reshape(spans, nbrs, length, width)


def solution(mesh):
    sizes = mesh.shape
    in_specs = (
        P(("cx", "cy"), "tp", None),
        P(("cx", "cy"), None, None),
        P(("cx", "cy"), None),
        P(None, ("cx", "cy"), "tp"),
        P(None, "tp", ("cx", "cy")),
        P(),
        P(("cx", "cy"), "tp"),
        P("tp", ("cx", "cy")),
    )
    out_specs = P(("cx", "cy"), "tp", None, None)
    nz = sizes["cx"]
    fits = sizes["cy"] == 2 and sizes["tp"] == 4 and nz & (nz - 1) == 0

    def body(*args):
        if fits and args[3].shape[1] % 16 == 0:
            return fast_body(nz, *args)
        return general_body(*args)

    return jax.shard_map(body, mesh=mesh, in_specs=in_specs, out_specs=out_specs, check_vma=False)
```
